8 devices in a mesh: dp: 1 (over z), vp: 8 (over y, x, core).
Axes of the slice: x: 2, y: 2, z: 1, core: 2. Of those that a mesh axis runs over, the one named last changes fastest.
Arguments:
- hidden: bfloat16 [128, 32, 4096], P('vp', 'dp')
- norm_gain: float32 [4096], replicated
- norm_bias: float32 [4096], replicated
- w_out: bfloat16 [4096, 51200], P(None, 'vp')
- labels: int32 [128, 32], P('vp', 'dp')
- loss_mask: float32 [128, 32], P('vp', 'dp')
Outputs:
- output 1: float32 [1], P('dp')
- output 2: bfloat16 [128, 32, 4096], P('vp', 'dp')
- output 3: float32 [4096, 51200], P('dp', 'vp')
- output 4: float32 [4096], P('dp')
- output 5: float32 [4096], P('dp')
All inputs are finite; a program needn't handle non-finite values.
Results may differ from the reference program's by a relative error of at most 0.001.
Values are sent between devices in bfloat16 or wider.
A program may use at most 1 GiB of HBM per device.

```python
import jax
import jax.numpy as jnp
from jax import lax

SEQ_DEV = 16
GROUP_SIZE = 8
BATCH_PART = 32
D_MODEL = 4096
VOCAB_SIZE = 50432
VOCAB_PAD = 51200
NORM_EPS = 1e-5
SEQ_LEN = SEQ_DEV * GROUP_SIZE
BLOCK_TOKENS = SEQ_DEV * BATCH_PART


def draw_labels(rng_key):
    key_pick, key_flat, key_upper, key_inner, key_skew = jax.random.split(rng_key, 5)
    tok_shape = (SEQ_LEN, BATCH_PART)
    flat_ids = jax.random.randint(key_flat, tok_shape, 0, VOCAB_SIZE)
    upper_one = jax.random.randint(key_upper, tok_shape, 1, VOCAB_SIZE + 1)
    upper_two = jax.random.randint(key_inner, tok_shape, 1, upper_one + 1)
    skew_ids = jax.random.randint(key_skew, tok_shape, 0, upper_two)
    pick_flat = jax.random.randint(key_pick, tok_shape, 0, 2)
    label_ids = jnp.where(pick_flat == 0, flat_ids, skew_ids)
    label_ids = label_ids.at[0, 0].set(VOCAB_SIZE - 1)
    return label_ids.at[SEQ_LEN - 1, BATCH_PART - 1].set(0)


def draw_mask(rng_key):
    mask_ids = jax.random.randint(rng_key, (SEQ_LEN, BATCH_PART), 0, 4)
    return (mask_ids > 0).astype(jnp.float32).at[0, 0].set(1.0)


def setup_inputs(seed: int = 0, part: int = 0) -> dict:
    root_key = jax.random.key(seed)
    shared_key, part_base = jax.random.split(root_key)
    part_key = jax.random.fold_in(part_base, part)
    key_w, key_g, key_c = jax.random.split(shared_key, 3)
    key_x, key_lab, key_mask = jax.random.split(part_key, 3)
    hidden = jax.random.normal(key_x, (SEQ_LEN, BATCH_PART, D_MODEL), jnp.float32).astype(jnp.bfloat16)
    norm_gain = 0.3 * jax.random.normal(key_g, (D_MODEL,), jnp.float32)
    norm_bias = 0.5 * jax.random.normal(key_c, (D_MODEL,), jnp.float32)
    w_out = (jax.random.normal(key_w, (D_MODEL, VOCAB_PAD), jnp.float32) * (2.0 / D_MODEL ** 0.5)).astype(jnp.bfloat16)
    labels = draw_labels(key_lab)
    loss_mask = draw_mask(key_mask)
    return {"hidden": hidden, "norm_gain": norm_gain, "norm_bias": norm_bias, "w_out": w_out, "labels": labels, "loss_mask": loss_mask}


def reference(hidden, norm_gain, norm_bias, w_out, labels, loss_mask):
    mask_total = jnp.sum(loss_mask)
    x_blocks = hidden.reshape(GROUP_SIZE, BLOCK_TOKENS, D_MODEL)
    lab_blocks = labels.reshape(GROUP_SIZE, BLOCK_TOKENS)
    mask_blocks = loss_mask.reshape(GROUP_SIZE, BLOCK_TOKENS)
    col_ids = jnp.arange(VOCAB_PAD, dtype=jnp.int32)

    def block_step(acc_state, block_in):
        grad_w, loss_sum, gain_sum, bias_sum = acc_state
        x_blk, lab_blk, mask_blk = block_in
        x_float = x_blk.astype(jnp.float32)
        tok_mean = jnp.mean(x_float, axis=-1, keepdims=True)
        centered = x_float - tok_mean
        inv_std = lax.rsqrt(jnp.mean(centered * centered, axis=-1, keepdims=True) + NORM_EPS)
        normed = centered * inv_std
        h_blk = (normed * (1.0 + norm_gain) + norm_bias).astype(jnp.bfloat16)
        logits = jnp.dot(h_blk, w_out, preferred_element_type=jnp.float32)
        row_max = jnp.max(logits, axis=-1, keepdims=True)
        exp_shift = jnp.exp(logits - row_max)
        sum_exp = jnp.sum(exp_shift, axis=-1, keepdims=True)
        is_label = (col_ids[None, :] == lab_blk[:, None]).astype(jnp.float32)
        target = jnp.sum(logits * is_label, axis=-1)
        tok_loss = row_max[:, 0] + jnp.log(sum_exp[:, 0]) - target
        tok_weight = mask_blk / mask_total
        grad_logits = ((exp_shift / sum_exp - is_label) * tok_weight[:, None]).astype(jnp.bfloat16)
        grad_w = grad_w + jnp.dot(h_blk.T, grad_logits, preferred_element_type=jnp.float32)
        grad_h = jnp.dot(grad_logits, w_out.T, preferred_element_type=jnp.float32)
        gain_sum = gain_sum + jnp.sum(grad_h * normed, axis=0)
        bias_sum = bias_sum + jnp.sum(grad_h, axis=0)
        scaled = grad_h * (1.0 + norm_gain)
        grad_x = inv_std * (scaled - jnp.mean(scaled, axis=-1, keepdims=True) - normed * jnp.mean(scaled * normed, axis=-1, keepdims=True))
        loss_sum = loss_sum + jnp.sum(mask_blk * tok_loss)
        return (grad_w, loss_sum, gain_sum, bias_sum), grad_x.astype(jnp.bfloat16)

    init_state = (jnp.zeros((D_MODEL, VOCAB_PAD), jnp.float32), jnp.zeros((), jnp.float32), jnp.zeros((D_MODEL,), jnp.float32), jnp.zeros((D_MODEL,), jnp.float32))
    final_state, grad_x = lax.scan(block_step, init_state, (x_blocks, lab_blocks, mask_blocks))
    grad_w, loss_sum, gain_sum, bias_sum = final_state
    loss = (loss_sum / mask_total).reshape(1)
    return loss, grad_x.reshape(SEQ_LEN, BATCH_PART, D_MODEL), grad_w, gain_sum, bias_sum
```

```python
import functools

import jax
import jax.numpy as jnp
from jax import lax
from jax.experimental import pallas as pl
from jax.experimental.pallas import tpu as pltpu
from jax.sharding import PartitionSpec as P

NORM_EPS = 1e-5
MESH = pl.DeviceIdType.MESH
F32, BF16 = jnp.float32, jnp.bfloat16
VMEM_CAP = 66_000_000
STRIP = 64


def norm_kernel(x_ref, g_ref, c_ref, h_ref):
    x = x_ref[...].astype(F32)
    cen = x - jnp.mean(x, axis=-1, keepdims=True)
    inv = lax.rsqrt(jnp.mean(cen * cen, axis=-1, keepdims=True) + NORM_EPS)
    h_ref[...] = (cen * inv * (1.0 + g_ref[...]) + c_ref[...]).astype(BF16)


def norm_fwd(x, g, c):
    rows, d = x.shape
    bm = 128
    vec = pl.BlockSpec((1, d), lambda i: (0, 0))
    return pl.pallas_call(
        norm_kernel,
        grid=(rows // bm,),
        in_specs=[pl.BlockSpec((bm, d), lambda i: (i, 0)), vec, vec],
        out_specs=pl.BlockSpec((bm, d), lambda i: (i, 0)),
        out_shape=jax.ShapeDtypeStruct((rows, d), BF16),
        compiler_params=pltpu.CompilerParams(vmem_limit_bytes=VMEM_CAP),
        name="norm_fwd",
    )(x, g, c)


def logits_kernel(nv, h_ref, w_ref, z_ref, m_ref, s_ref, mx, sm):
    v = pl.program_id(1)
    bm, bn = z_ref.shape
    cut = 256

    @pl.when(v == 0)
    def _():
        mx[...] = jnp.full_like(mx, -jnp.inf)
        sm[...] = jnp.zeros_like(sm)

    for p in range(bn // cut):
        part = slice(cut * p, cut * (p + 1))
        z_ref[:, part] = jnp.dot(h_ref[...], w_ref[:, part], preferred_element_type=F32)
        for r in range(0, bm, STRIP):
            rows = slice(r, r + STRIP)
            zs = [z_ref[rows, c : c + 128] for c in range(cut * p, cut * (p + 1), 128)]
            old = mx[rows]
            new = functools.reduce(jnp.maximum, zs, old)
            acc = sm[rows] * jnp.exp(old - new)
            for z in zs:
                acc = acc + jnp.exp(z - new)
            mx[rows] = new
            sm[rows] = acc

    @pl.when(v == nv - 1)
    def _():
        new = mx[...]
        row_m = jnp.max(new, axis=1, keepdims=True)
        row_s = jnp.sum(sm[...] * jnp.exp(new - row_m), axis=1, keepdims=True)
        for j in range(bm // 128):
            part = slice(128 * j, 128 * (j + 1))
            m_ref[j : j + 1, :] = jnp.broadcast_to(row_m[part], (128, 128)).T[:1]
            s_ref[j : j + 1, :] = jnp.broadcast_to(row_s[part], (128, 128)).T[:1]


def logits_fwd(h, w):
    t, d = h.shape
    vl = w.shape[1]
    bm, bn = 1024, 1280
    stat = pl.BlockSpec((bm // 128, 128), lambda i, v: (i, 0))
    stat_shape = jax.ShapeDtypeStruct((t // 128, 128), F32)
    return pl.pallas_call(
        functools.partial(logits_kernel, vl // bn),
        grid=(t // bm, vl // bn),
        in_specs=[pl.BlockSpec((bm, d), lambda i, v: (i, 0)), pl.BlockSpec((d, bn), lambda i, v: (0, v))],
        out_specs=[pl.BlockSpec((bm, bn), lambda i, v: (i, v)), stat, stat],
        out_shape=[jax.ShapeDtypeStruct((t, vl), F32), stat_shape, stat_shape],
        scratch_shapes=[pltpu.VMEM((bm, 128), F32), pltpu.VMEM((bm, 128), F32)],
        compiler_params=pltpu.CompilerParams(vmem_limit_bytes=VMEM_CAP),
        cost_estimate=pl.CostEstimate(flops=2 * t * d * vl, bytes_accessed=4 * t * vl, transcendentals=0),
        name="logits_fwd",
    )(h, w)


def exchange_kernel(n, post, n_out, x_ref, *rest):
    outs, (recv, send_sem, recv_sem) = rest[:n_out], rest[n_out:]
    me = lax.axis_index("vp")
    zero = lax.axis_index("dp")
    barrier = pltpu.get_barrier_semaphore()
    for k in range(1, n):
        pl.semaphore_signal(barrier, inc=1, device_id=(zero, lax.rem(me + k, n)), device_id_type=MESH)
    pl.semaphore_wait(barrier, n - 1)
    copies = []
    for k in range(1, n):
        copy = pltpu.make_async_remote_copy(
            src_ref=x_ref,
            dst_ref=recv.at[me],
            send_sem=send_sem.at[k],
            recv_sem=recv_sem.at[k],
            device_id=(zero, lax.rem(me + k, n)),
            device_id_type=MESH,
        )
        copy.start()
        copies.append(copy)
    recv[me] = x_ref[...]
    for copy in copies:
        copy.wait()
    post([recv[k] for k in range(n)], outs)


def exchange(x, n, post, out_shapes, cid, name):
    return pl.pallas_call(
        functools.partial(exchange_kernel, n, post, len(out_shapes)),
        in_specs=[pl.BlockSpec(memory_space=pltpu.VMEM)],
        out_specs=[pl.BlockSpec(memory_space=pltpu.VMEM)] * len(out_shapes),
        out_shape=out_shapes,
        scratch_shapes=[
            pltpu.VMEM((n,) + x.shape, x.dtype),
            pltpu.SemaphoreType.DMA((n,)),
            pltpu.SemaphoreType.DMA((n,)),
        ],
        compiler_params=pltpu.CompilerParams(collective_id=cid, has_side_effects=True),
        name=name,
    )(x)


def stats_post(rows, own, parts, outs):
    m_ref, a_ref, lab_ref, misc_ref = outs
    top = parts[0][:rows]
    for p in parts[1:]:
        top = jnp.maximum(top, p[:rows])
    tot = parts[0][rows : 2 * rows] * jnp.exp(parts[0][:rows] - top)
    for p in parts[1:]:
        tot = tot + p[rows : 2 * rows] * jnp.exp(p[:rows] - top)
    lab = jnp.concatenate([p[2 * rows : 2 * rows + own] for p in parts], axis=0)
    mask = jnp.where(lab >= 0.0, 1.0, 0.0)
    count = jnp.sum(mask)
    m_ref[...] = top
    a_ref[...] = mask / count / tot
    lab_ref[...] = lab
    misc_ref[0:8, :] = jnp.full((8, 128), 1.0, F32) / count
    misc_ref[8:16, :] = jnp.full((8, 128), jnp.sum(mask * (top + jnp.log(tot))), F32)


def grad_h_kernel(nk, nn, z_ref, m_ref, a_ref, lab_ref, inv_ref, w_ref, *rest):
    dh_ref, dz_ref, t_ref, dz_s = rest[-4:]
    i = pl.program_id(0)
    groups, _, rows, bk = z_ref.shape
    bn = w_ref.shape[0]
    cut = 256
    contract = (((1,), (1,)), ((), ()))

    def make_dz():
        inv = jnp.broadcast_to(inv_ref[0:1, :], (STRIP, 128))
        lane = lax.broadcasted_iota(jnp.int32, (STRIP, 128), 1)
        hit_sum = jnp.zeros((STRIP, 128), F32)
        lanes = [(lane + (i * bk + 128 * j)).astype(F32) for j in range(bk // 128)]
        for grp in range(groups):
            for r in range(0, rows, STRIP):
                part = slice(r, r + STRIP)
                m, a, lab = m_ref[grp, 0, part], a_ref[grp, 0, part], lab_ref[grp, 0, part]
                for j in range(bk // 128):
                    cols = slice(128 * j, 128 * (j + 1))
                    z = z_ref[grp, 0, part, cols]
                    hit = lab == lanes[j]
                    hit_sum = hit_sum + jnp.where(hit, z, 0.0)
                    dz = (jnp.exp(z - m) * a - jnp.where(hit, inv, 0.0)).astype(BF16)
                    dz_s[i, grp * rows + r : grp * rows + r + STRIP, cols] = dz
                    dz_ref[grp, 0, part, cols] = dz
        for r in range(0, STRIP, 8):
            t_ref[...] += hit_sum[r : r + 8]

    def product():
        k = lax.rem(i - 1, nk)
        keep = jnp.where(k == 0, 0.0, 1.0)
        for p in range(bn // cut):
            part = lax.dot_general(
                dz_s[k], w_ref[cut * p : cut * (p + 1), :], contract, preferred_element_type=F32
            )
            cols = slice(cut * p, cut * (p + 1))
            dh_ref[:, cols] = jnp.where(k == 0, 0.0, dh_ref[:, cols]) + part

    @pl.when(i == 0)
    def _():
        t_ref[...] = jnp.zeros_like(t_ref)
        make_dz()

    @pl.when((i > 0) & (i < nk))
    def _():
        product()
        make_dz()

    @pl.when(i >= nk)
    def _():
        product()


def grad_h_chunk(z4, m4, a4, lab4, inv, w, dz4, c):
    groups, _, rows, vl = z4.shape
    d = w.shape[0]
    bn, bk = 1024, 1280
    nk, nn = vl // bk, d // bn
    t = groups * rows
    tile = pl.BlockSpec((groups, 1, rows, bk), lambda i: (0, c, 0, jnp.minimum(i, nk - 1)))
    col = pl.BlockSpec((groups, 1, rows, 128), lambda i: (0, c, 0, 0))
    small = pl.BlockSpec((8, 128), lambda i: (0, 0))
    in_specs = [tile, col, col, col, small, pl.BlockSpec((bn, bk), lambda i: (jnp.maximum(i - 1, 0) // nk, lax.rem(jnp.maximum(i - 1, 0), nk)))]
    args = [z4, m4, a4, lab4, inv, w]
    aliases = {}
    if dz4 is not None:
        in_specs.append(pl.BlockSpec(memory_space=pl.ANY))
        aliases = {len(args): 1}
        args.append(dz4)
    return pl.pallas_call(
        functools.partial(grad_h_kernel, nk, nn),
        grid=(nk * nn + 1,),
        in_specs=in_specs,
        out_specs=[pl.BlockSpec((t, bn), lambda i: (0, jnp.maximum(i - 1, 0) // nk)), tile, small],
        out_shape=[
            jax.ShapeDtypeStruct((t, d), F32),
            jax.ShapeDtypeStruct(z4.shape, BF16),
            jax.ShapeDtypeStruct((8, 128), F32),
        ],
        scratch_shapes=[pltpu.VMEM((nk, t, bk), BF16)],
        input_output_aliases=aliases,
        compiler_params=pltpu.CompilerParams(vmem_limit_bytes=VMEM_CAP),
        cost_estimate=pl.CostEstimate(flops=2 * t * d * vl, bytes_accessed=4 * t * vl, transcendentals=0),
        name="grad_h",
    )(*args)


def grad_w_kernel(h_ref, dz_ref, out_ref):
    out_ref[...] = lax.dot_general(h_ref[...], dz_ref[...], (((0,), (0,)), ((), ())), preferred_element_type=F32)


def grad_w_call(h, dz):
    t, d = h.shape
    vl = dz.shape[1]
    bm, bn = 1024, 1280
    return pl.pallas_call(
        grad_w_kernel,
        grid=(vl // bn, d // bm),
        in_specs=[pl.BlockSpec((t, bm), lambda v, i: (0, i)), pl.BlockSpec((t, bn), lambda v, i: (0, v))],
        out_specs=pl.BlockSpec((bm, bn), lambda v, i: (i, v)),
        out_shape=jax.ShapeDtypeStruct((d, vl), F32),
        compiler_params=pltpu.CompilerParams(vmem_limit_bytes=VMEM_CAP),
        cost_estimate=pl.CostEstimate(flops=2 * t * d * vl, bytes_accessed=4 * d * vl, transcendentals=0),
        name="grad_w",
    )(h, dz)


def norm_bwd_kernel(nc, x_ref, g_ref, *rest):
    dh_refs, dx_ref, sums_ref = rest[:nc], rest[nc], rest[nc + 1]
    rows, d = dh_refs[0].shape
    gain = 1.0 + g_ref[...]
    step = 32
    for c in range(nc):
        def body(i, sums, c=c):
            part = pl.ds(pl.multiple_of(i * step, step), step)
            x = x_ref[pl.ds(pl.multiple_of(c * rows + i * step, step), step), :].astype(F32)
            dh = dh_refs[c][part, :]
            cen = x - jnp.mean(x, axis=-1, keepdims=True)
            inv = lax.rsqrt(jnp.mean(cen * cen, axis=-1, keepdims=True) + NORM_EPS)
            nrm = cen * inv
            q = dh * gain
            q_mean = jnp.mean(q, axis=-1, keepdims=True)
            qn_mean = jnp.mean(q * nrm, axis=-1, keepdims=True)
            dx = inv * (q - q_mean - nrm * qn_mean)
            dx_ref[pl.ds(pl.multiple_of(c * rows + i * step, step), step), :] = dx.astype(BF16)
            sums_ref[0:8, :] += jnp.sum((dh * nrm).reshape(step // 8, 8, d), axis=0)
            sums_ref[8:16, :] += jnp.sum(dh.reshape(step // 8, 8, d), axis=0)
            return sums
        if c == 0:
            sums_ref[...] = jnp.zeros_like(sums_ref)
        lax.fori_loop(0, rows // step, body, 0)


def norm_bwd(x, g, dhs):
    rows, d = x.shape
    vm = pl.BlockSpec(memory_space=pltpu.VMEM)
    return pl.pallas_call(
        functools.partial(norm_bwd_kernel, len(dhs)),
        in_specs=[vm] * (2 + len(dhs)),
        out_specs=[vm, vm],
        out_shape=[jax.ShapeDtypeStruct((rows, d), BF16), jax.ShapeDtypeStruct((16, d), F32)],
        compiler_params=pltpu.CompilerParams(vmem_limit_bytes=VMEM_CAP),
        name="norm_bwd",
    )(x, g, *dhs)


def final_post(rows, parts, outs):
    tot = parts[0]
    for p in parts[1:]:
        tot = tot + p
    outs[0][...] = tot[:rows]
    outs[1][...] = jnp.full((8, 128), jnp.sum(tot[rows : rows + 8]), F32)


def solution(mesh):
    n = mesh.shape["vp"]

    def per_device(hidden, norm_gain, norm_bias, w, labels, loss_mask):
        s_loc, b_loc, d = hidden.shape
        rows = s_loc * b_loc
        t = rows * n
        vl = w.shape[1]
        nc = rows // 128
        x = hidden.reshape(rows, d)
        g = norm_gain.reshape(1, d)
        h_own = norm_fwd(x, g, norm_bias.reshape(1, d))
        h = lax.all_gather(h_own, "vp", axis=0, tiled=True)
        z, m_loc, s_loc_sum = logits_fwd(h, w)

        lab_own = jnp.where(loss_mask > 0.0, labels, -1).astype(F32).reshape(nc, 128)
        stat_rows = t // 128
        packed = jnp.concatenate([m_loc, s_loc_sum, lab_own, jnp.zeros((8 - nc % 8, 128), F32)], axis=0)
        compact = jax.ShapeDtypeStruct((stat_rows, 128), F32)
        m, a, lab, misc = exchange(
            packed,
            n,
            functools.partial(stats_post, stat_rows, nc),
            [compact, compact, compact, jax.ShapeDtypeStruct((16, 128), F32)],
            0,
            "stats_exchange",
        )
        col_start = (lax.axis_index("vp") * vl).astype(F32)

        def wide(v):
            return jnp.broadcast_to(v[:, :, None], (stat_rows, 128, 128)).reshape(n, nc, 128, 128)

        m4, a4, lab4 = wide(m), wide(a), wide(lab - col_start)
        z4 = z.reshape(n, nc, 128, vl)
        inv = misc[:8]
        dz4, dhs, hits = None, [], []
        for c in range(nc):
            dh_c, dz4, hit = grad_h_chunk(z4, m4, a4, lab4, inv, w, dz4, c)
            hits.append(hit)
            dhs.append(lax.psum_scatter(dh_c, "vp", scatter_dimension=0, tiled=True))
        grad_w = grad_w_call(h, dz4.reshape(t, vl))
        grad_x, sums = norm_bwd(x, g, dhs)
        vecs = jnp.sum(sums.reshape(2, 8, d), axis=1).reshape(2 * d // 128, 128)
        packed2 = jnp.concatenate([vecs, sum(hits)], axis=0)
        vrows = 2 * d // 128
        out_vec, hit_tot = exchange(
            packed2,
            n,
            functools.partial(final_post, vrows),
            [jax.ShapeDtypeStruct((vrows, 128), F32), jax.ShapeDtypeStruct((8, 128), F32)],
            1,
            "final_exchange",
        )
        loss = (misc[8, 0] - hit_tot[0, 0]) * misc[0, 0]
        out_vec = out_vec.reshape(2, d)
        return loss.reshape(1), grad_x.reshape(hidden.shape), grad_w, out_vec[0], out_vec[1]

    tok_spec = P("vp", "dp")
    return jax.shard_map(
        per_device,
        mesh=mesh,
        in_specs=(P("vp", "dp", None), P(None), P(None), P(None, "vp"), tok_spec, tok_spec),
        out_specs=(P("dp"), P("vp", "dp", None), P("dp", "vp"), P("dp"), P("dp")),
        check_vma=False,
    )
```

```python
import functools

import jax
import jax.numpy as jnp
from jax import lax
from jax.experimental import pallas as pl
from jax.experimental.pallas import tpu as pltpu
from jax.sharding import PartitionSpec as P

NORM_EPS = 1e-5
MESH = pl.DeviceIdType.MESH
F32, BF16 = jnp.float32, jnp.bfloat16
VMEM_CAP = 66_000_000
STRIP = 64


def norm_kernel(x_ref, g_ref, c_ref, h_ref):
    x = x_ref[...].astype(F32)
    cen = x - jnp.mean(x, axis=-1, keepdims=True)
    inv = lax.rsqrt(jnp.mean(cen * cen, axis=-1, keepdims=True) + NORM_EPS)
    h_ref[...] = (cen * inv * (1.0 + g_ref[...]) + c_ref[...]).astype(BF16)


def norm_fwd(x, g, c):
    rows, d = x.shape
    bm = 128
    vec = pl.BlockSpec((1, d), lambda i: (0, 0))
    return pl.pallas_call(
        norm_kernel,
        grid=(rows // bm,),
        in_specs=[pl.BlockSpec((bm, d), lambda i: (i, 0)), vec, vec],
        out_specs=pl.BlockSpec((bm, d), lambda i: (i, 0)),
        out_shape=jax.ShapeDtypeStruct((rows, d), BF16),
        compiler_params=pltpu.CompilerParams(vmem_limit_bytes=VMEM_CAP),
        name="norm_fwd",
    )(x, g, c)


def gather_logits_kernel(nv, own_ref, w_ref, all_ref, z_ref, m_ref, s_ref, hbuf, zbuf, mx, sm, send_sem, recv_sem, load_sem, own_sem, z_sem):
    i = pl.program_id(0)
    u, v = lax.div(i, nv), lax.rem(i, nv)
    last = 4 * nv - 1
    blk = own_ref.shape[0]
    half = blk // 2
    bm, bn = zbuf.shape[1:]
    cut = 256
    zero = lax.axis_index("dp")
    me = lax.axis_index("vp")
    core = (zero, me + 1 - 2 * lax.rem(me, 2))
    over_x = (zero, me + 2 - 4 * lax.rem(lax.div(me, 2), 2))
    over_y = (zero, me + 4 - 8 * lax.div(me, 4))

    def piece(slot, part):
        return pl.ds(slot * blk + max(part, 0) * half, blk if part < 0 else half)

    def remote(k, src, dst, to):
        return pltpu.make_async_remote_copy(
            src_ref=src,
            dst_ref=all_ref.at[dst],
            send_sem=send_sem.at[k],
            recv_sem=recv_sem.at[k],
            device_id=to,
            device_id_type=MESH,
        )

    def forward(k, slot, part, slot_to, to):
        return remote(k, all_ref.at[piece(slot, part)], piece(slot_to, part), to)

    copies = [
        remote(0, own_ref, piece(1, -1), core),
        remote(1, own_ref.at[piece(0, 0)], piece(2, 0), over_x),
        remote(2, own_ref.at[piece(0, 0)], piece(4, 0), over_y),
        remote(3, own_ref.at[piece(0, 1)], piece(2, 1), over_x),
        remote(4, own_ref.at[piece(0, 1)], piece(4, 1), over_y),
        forward(5, 2, 0, 3, core),
        forward(6, 4, 0, 5, core),
        forward(7, 4, 0, 6, over_x),
        forward(8, 2, 1, 3, core),
        forward(9, 4, 1, 5, core),
        forward(10, 2, 1, 6, over_y),
        forward(11, 6, -1, 7, core),
    ]

    def load(src, b, q, count):
        return pltpu.make_async_copy(src, hbuf.at[b, pl.ds(q * half, count * half)], load_sem.at[b, q])

    def load_slot(slot, part, b, q):
        return load(all_ref.at[piece(slot, part)], b, q, 2 if part < 0 else 1)

    keep_own = pltpu.make_async_copy(hbuf.at[0, pl.ds(0, blk)], all_ref.at[piece(0, -1)], own_sem)

    @pl.when(i == 0)
    def _():
        own_load = load(own_ref, 0, 0, 2)
        own_load.start()
        barrier = pltpu.get_barrier_semaphore()
        for to in (core, over_x, over_y):
            pl.semaphore_signal(barrier, inc=1, device_id=to, device_id_type=MESH)
        pl.semaphore_wait(barrier, 3)
        for k in range(5):
            copies[k].start()
        own_load.wait()
        keep_own.start()
        copies[0].wait_recv()
        other = load_slot(1, -1, 0, 2)
        other.start()
        other.wait()

    @pl.when(i == nv - 1)
    def _():
        keep_own.wait()
        for k in (1, 2):
            copies[k].wait_recv()
        for k in (5, 6, 7):
            copies[k].start()
        load_slot(2, 0, 1, 0).start()
        load_slot(4, 0, 1, 2).start()

    @pl.when(i == nv)
    def _():
        for k in (5, 6):
            copies[k].wait_recv()
        load_slot(3, 0, 1, 1).start()
        load_slot(5, 0, 1, 3).start()
        for q in range(4):
            load_slot(2 + q, 0, 1, q).wait()

    @pl.when(i == 2 * nv - 2)
    def _():
        for k in (3, 4):
            copies[k].wait_recv()
        for k in (8, 9, 10):
            copies[k].start()
        load_slot(2, 1, 0, 0).start()
        load_slot(4, 1, 0, 2).start()

    @pl.when(i == 2 * nv)
    def _():
        for k in (8, 9):
            copies[k].wait_recv()
        load_slot(3, 1, 0, 1).start()
        load_slot(5, 1, 0, 3).start()
        for q in range(4):
            load_slot(2 + q, 1, 0, q).wait()

    @pl.when(i == 3 * nv - 2)
    def _():
        for k in (7, 10):
            copies[k].wait_recv()
        copies[11].start()
        load_slot(6, -1, 1, 0).start()

    @pl.when(i == 3 * nv)
    def _():
        copies[11].wait_recv()
        load_slot(7, -1, 1, 2).start()
        load_slot(6, -1, 1, 0).wait()
        load_slot(7, -1, 1, 2).wait()

    def row_of(unit, q):
        edge = (unit == 0) | (unit == 3)
        return jnp.where(edge, unit * 4 * half + q * half, (4 + 2 * q) * half + (unit - 1) * half)

    def put(step, q):
        row = pl.multiple_of(row_of(lax.div(step, nv), q), half)
        col = pl.multiple_of(lax.rem(step, nv) * bn, bn)
        b = lax.rem(step, 2)
        return pltpu.make_async_copy(
            zbuf.at[b, pl.ds(q * half, half)], z_ref.at[pl.ds(row, half), pl.ds(col, bn)], z_sem.at[b, q]
        )

    @pl.when(i >= 2)
    def _():
        for q in range(4):
            put(i - 2, q).wait()

    @pl.when(v == 0)
    def _():
        mx[...] = jnp.full_like(mx, -jnp.inf)
        sm[...] = jnp.zeros_like(sm)

    hb, zb = lax.rem(u, 2), lax.rem(i, 2)
    for p in range(bn // cut):
        part = slice(cut * p, cut * (p + 1))
        zbuf[zb, :, part] = jnp.dot(hbuf[hb], w_ref[:, part], preferred_element_type=F32)
        for r in range(0, bm, STRIP):
            rows = slice(r, r + STRIP)
            zs = [zbuf[zb, rows, c : c + 128] for c in range(cut * p, cut * (p + 1), 128)]
            old = mx[rows]
            new = functools.reduce(jnp.maximum, zs, old)
            acc = sm[rows] * jnp.exp(old - new)
            for z in zs:
                acc = acc + jnp.exp(z - new)
            mx[rows] = new
            sm[rows] = acc

    for q in range(4):
        put(i, q).start()

    @pl.when(v == nv - 1)
    def _():
        new = mx[...]
        row_m = jnp.max(new, axis=1, keepdims=True)
        row_s = jnp.sum(sm[...] * jnp.exp(new - row_m), axis=1, keepdims=True)
        per = half // 128
        for j in range(bm // 128):
            part = slice(128 * j, 128 * (j + 1))
            row = lax.div(row_of(u, j // per), 128) + j % per
            m_ref[pl.ds(row, 1), :] = jnp.broadcast_to(row_m[part], (128, 128)).T[:1]
            s_ref[pl.ds(row, 1), :] = jnp.broadcast_to(row_s[part], (128, 128)).T[:1]

    @pl.when(i == last)
    def _():
        for k in range(12):
            copies[k].wait_send()
        for q in range(4):
            put(i - 1, q).wait()
            put(i, q).wait()


def gather_logits(h_own, w, n):
    blk, d = h_own.shape
    t = n * blk
    vl = w.shape[1]
    bm, bn = 2 * blk, 1280
    nv = vl // bn
    stat = pl.BlockSpec((t // 128, 128), lambda i: (0, 0))
    stat_shape = jax.ShapeDtypeStruct((t // 128, 128), F32)
    hbm = pl.BlockSpec(memory_space=pl.ANY)
    return pl.pallas_call(
        functools.partial(gather_logits_kernel, nv),
        grid=(4 * nv,),
        in_specs=[hbm, pl.BlockSpec((d, bn), lambda i: (0, lax.rem(i, nv)))],
        out_specs=[hbm, hbm, stat, stat],
        out_shape=[jax.ShapeDtypeStruct((t, d), BF16), jax.ShapeDtypeStruct((t, vl), F32), stat_shape, stat_shape],
        scratch_shapes=[
            pltpu.VMEM((2, bm, d), BF16),
            pltpu.VMEM((2, bm, bn), F32),
            pltpu.VMEM((bm, 128), F32),
            pltpu.VMEM((bm, 128), F32),
            pltpu.SemaphoreType.DMA((12,)),
            pltpu.SemaphoreType.DMA((12,)),
            pltpu.SemaphoreType.DMA((2, 4)),
            pltpu.SemaphoreType.DMA,
            pltpu.SemaphoreType.DMA((2, 4)),
        ],
        compiler_params=pltpu.CompilerParams(
            vmem_limit_bytes=VMEM_CAP, collective_id=2, has_side_effects=True
        ),
        cost_estimate=pl.CostEstimate(flops=2 * t * d * vl, bytes_accessed=4 * t * vl, transcendentals=0),
        name="gather_logits",
    )(h_own, w)


def exchange_kernel(n, post, n_out, x_ref, *rest):
    outs, (recv, send_sem, recv_sem) = rest[:n_out], rest[n_out:]
    me = lax.axis_index("vp")
    zero = lax.axis_index("dp")
    barrier = pltpu.get_barrier_semaphore()
    for k in range(1, n):
        pl.semaphore_signal(barrier, inc=1, device_id=(zero, lax.rem(me + k, n)), device_id_type=MESH)
    pl.semaphore_wait(barrier, n - 1)
    copies = []
    for k in range(1, n):
        copy = pltpu.make_async_remote_copy(
            src_ref=x_ref,
            dst_ref=recv.at[me],
            send_sem=send_sem.at[k],
            recv_sem=recv_sem.at[k],
            device_id=(zero, lax.rem(me + k, n)),
            device_id_type=MESH,
        )
        copy.start()
        copies.append(copy)
    recv[me] = x_ref[...]
    for copy in copies:
        copy.wait()
    post([recv[k] for k in range(n)], outs)


def exchange(x, n, post, out_shapes, cid, name):
    return pl.pallas_call(
        functools.partial(exchange_kernel, n, post, len(out_shapes)),
        in_specs=[pl.BlockSpec(memory_space=pltpu.VMEM)],
        out_specs=[pl.BlockSpec(memory_space=pltpu.VMEM)] * len(out_shapes),
        out_shape=out_shapes,
        scratch_shapes=[
            pltpu.VMEM((n,) + x.shape, x.dtype),
            pltpu.SemaphoreType.DMA((n,)),
            pltpu.SemaphoreType.DMA((n,)),
        ],
        compiler_params=pltpu.CompilerParams(collective_id=cid, has_side_effects=True),
        name=name,
    )(x)


def stats_post(rows, own, parts, outs):
    m_ref, a_ref, lab_ref, misc_ref = outs
    top = parts[0][:rows]
    for p in parts[1:]:
        top = jnp.maximum(top, p[:rows])
    tot = parts[0][rows : 2 * rows] * jnp.exp(parts[0][:rows] - top)
    for p in parts[1:]:
        tot = tot + p[rows : 2 * rows] * jnp.exp(p[:rows] - top)
    lab = jnp.concatenate([p[2 * rows : 2 * rows + own] for p in parts], axis=0)
    mask = jnp.where(lab >= 0.0, 1.0, 0.0)
    count = jnp.sum(mask)
    m_ref[...] = top
    a_ref[...] = mask / count / tot
    lab_ref[...] = lab
    misc_ref[0:8, :] = jnp.full((8, 128), 1.0, F32) / count
    misc_ref[8:16, :] = jnp.full((8, 128), jnp.sum(mask * (top + jnp.log(tot))), F32)


def grad_h_kernel(nk, me_ref, z_ref, m_ref, a_ref, lab_ref, inv_ref, w_ref, *rest):
    dh_ref, dz_ref, t_ref, dz_s = rest[-4:]
    i = pl.program_id(0)
    groups, _, rows, bk = z_ref.shape
    bn = w_ref.shape[0]
    cut = 256
    contract = (((1,), (1,)), ((), ()))

    def make_dz():
        inv = jnp.broadcast_to(inv_ref[0:1, :], (STRIP, 128))
        lane = lax.broadcasted_iota(jnp.int32, (STRIP, 128), 1)
        hit_sum = jnp.zeros((STRIP, 128), F32)
        lanes = [(lane + (i * bk + 128 * j)).astype(F32) for j in range(bk // 128)]
        for grp in range(groups):
            slot = lax.bitwise_xor(me_ref[0], grp)
            for r in range(0, rows, STRIP):
                part = slice(r, r + STRIP)
                m, a, lab = m_ref[grp, 0, part], a_ref[grp, 0, part], lab_ref[grp, 0, part]
                for j in range(bk // 128):
                    cols = slice(128 * j, 128 * (j + 1))
                    z = z_ref[slot, 0, part, cols]
                    hit = lab == lanes[j]
                    hit_sum = hit_sum + jnp.where(hit, z, 0.0)
                    dz = (jnp.exp(z - m) * a - jnp.where(hit, inv, 0.0)).astype(BF16)
                    dz_s[i, grp * rows + r : grp * rows + r + STRIP, cols] = dz
                    dz_ref[slot, 0, part, cols] = dz
        for r in range(0, STRIP, 8):
            t_ref[...] += hit_sum[r : r + 8]

    def product():
        k = lax.rem(i - 1, nk)
        keep = jnp.where(k == 0, 0.0, 1.0)
        for p in range(bn // cut):
            part = lax.dot_general(
                dz_s[k], w_ref[cut * p : cut * (p + 1), :], contract, preferred_element_type=F32
            )
            cols = slice(cut * p, cut * (p + 1))
            dh_ref[:, cols] = jnp.where(k == 0, 0.0, dh_ref[:, cols]) + part

    @pl.when(i == 0)
    def _():
        t_ref[...] = jnp.zeros_like(t_ref)
        make_dz()

    @pl.when((i > 0) & (i < nk))
    def _():
        product()
        make_dz()

    @pl.when(i >= nk)
    def _():
        product()


def grad_h_chunk(me, z4, m4, a4, lab4, inv, w, dz4, c):
    groups, _, rows, vl = z4.shape
    d = w.shape[0]
    bn, bk = 1024, 1280
    nk, nn = vl // bk, d // bn
    t = groups * rows
    tile = pl.BlockSpec((groups, 1, rows, bk), lambda i: (0, c, 0, jnp.minimum(i, nk - 1)))
    col = pl.BlockSpec((groups, 1, rows, 128), lambda i: (0, c, 0, 0))
    small = pl.BlockSpec((8, 128), lambda i: (0, 0))
    in_specs = [pl.BlockSpec(memory_space=pltpu.SMEM), tile, col, col, col, small, pl.BlockSpec((bn, bk), lambda i: (jnp.maximum(i - 1, 0) // nk, lax.rem(jnp.maximum(i - 1, 0), nk)))]
    args = [me, z4, m4, a4, lab4, inv, w]
    aliases = {}
    if dz4 is not None:
        in_specs.append(pl.BlockSpec(memory_space=pl.ANY))
        aliases = {len(args): 1}
        args.append(dz4)
    return pl.pallas_call(
        functools.partial(grad_h_kernel, nk),
        grid=(nk * nn + 1,),
        in_specs=in_specs,
        out_specs=[pl.BlockSpec((t, bn), lambda i: (0, jnp.maximum(i - 1, 0) // nk)), tile, small],
        out_shape=[
            jax.ShapeDtypeStruct((t, d), F32),
            jax.ShapeDtypeStruct(z4.shape, BF16),
            jax.ShapeDtypeStruct((8, 128), F32),
        ],
        scratch_shapes=[pltpu.VMEM((nk, t, bk), BF16)],
        input_output_aliases=aliases,
        compiler_params=pltpu.CompilerParams(vmem_limit_bytes=VMEM_CAP),
        cost_estimate=pl.CostEstimate(flops=2 * t * d * vl, bytes_accessed=4 * t * vl, transcendentals=0),
        name="grad_h",
    )(*args)


def grad_w_kernel(h_ref, dz_ref, out_ref):
    out_ref[...] = lax.dot_general(h_ref[...], dz_ref[...], (((0,), (0,)), ((), ())), preferred_element_type=F32)


def grad_w_call(h, dz):
    t, d = h.shape
    vl = dz.shape[1]
    bm, bn = 1024, 1280
    return pl.pallas_call(
        grad_w_kernel,
        grid=(vl // bn, d // bm),
        in_specs=[pl.BlockSpec((t, bm), lambda v, i: (0, i)), pl.BlockSpec((t, bn), lambda v, i: (0, v))],
        out_specs=pl.BlockSpec((bm, bn), lambda v, i: (i, v)),
        out_shape=jax.ShapeDtypeStruct((d, vl), F32),
        compiler_params=pltpu.CompilerParams(vmem_limit_bytes=VMEM_CAP),
        cost_estimate=pl.CostEstimate(flops=2 * t * d * vl, bytes_accessed=4 * d * vl, transcendentals=0),
        name="grad_w",
    )(h, dz)


def norm_bwd_kernel(nc, x_ref, g_ref, *rest):
    dh_refs, dx_ref, sums_ref = rest[:nc], rest[nc], rest[nc + 1]
    rows, d = dh_refs[0].shape
    gain = 1.0 + g_ref[...]
    step = 32
    for c in range(nc):
        def body(i, sums, c=c):
            part = pl.ds(pl.multiple_of(i * step, step), step)
            x = x_ref[pl.ds(pl.multiple_of(c * rows + i * step, step), step), :].astype(F32)
            dh = dh_refs[c][part, :]
            cen = x - jnp.mean(x, axis=-1, keepdims=True)
            inv = lax.rsqrt(jnp.mean(cen * cen, axis=-1, keepdims=True) + NORM_EPS)
            nrm = cen * inv
            q = dh * gain
            q_mean = jnp.mean(q, axis=-1, keepdims=True)
            qn_mean = jnp.mean(q * nrm, axis=-1, keepdims=True)
            dx = inv * (q - q_mean - nrm * qn_mean)
            dx_ref[pl.ds(pl.multiple_of(c * rows + i * step, step), step), :] = dx.astype(BF16)
            sums_ref[0:8, :] += jnp.sum((dh * nrm).reshape(step // 8, 8, d), axis=0)
            sums_ref[8:16, :] += jnp.sum(dh.reshape(step // 8, 8, d), axis=0)
            return sums
        if c == 0:
            sums_ref[...] = jnp.zeros_like(sums_ref)
        lax.fori_loop(0, rows // step, body, 0)


def norm_bwd(x, g, dhs):
    rows, d = x.shape
    vm = pl.BlockSpec(memory_space=pltpu.VMEM)
    return pl.pallas_call(
        functools.partial(norm_bwd_kernel, len(dhs)),
        in_specs=[vm] * (2 + len(dhs)),
        out_specs=[vm, vm],
        out_shape=[jax.ShapeDtypeStruct((rows, d), BF16), jax.ShapeDtypeStruct((16, d), F32)],
        compiler_params=pltpu.CompilerParams(vmem_limit_bytes=VMEM_CAP),
        name="norm_bwd",
    )(x, g, *dhs)


def final_post(rows, parts, outs):
    tot = parts[0]
    for p in parts[1:]:
        tot = tot + p
    outs[0][...] = tot[:rows]
    outs[1][...] = jnp.full((8, 128), jnp.sum(tot[rows : rows + 8]), F32)


def solution(mesh):
    n = mesh.shape["vp"]

    def per_device(hidden, norm_gain, norm_bias, w, labels, loss_mask):
        s_loc, b_loc, d = hidden.shape
        rows = s_loc * b_loc
        t = rows * n
        vl = w.shape[1]
        nc = rows // 128
        x = hidden.reshape(rows, d)
        g = norm_gain.reshape(1, d)
        h_own = norm_fwd(x, g, norm_bias.reshape(1, d))
        h, z, m_slot, s_slot = gather_logits(h_own, w, n)
        me = lax.axis_index("vp")
        me_arr = me.reshape(1)

        def by_device(v):
            v = v.reshape(2, 2, 2, t // 128 // n, 128)
            for axis, bit in ((0, 4), (1, 2), (2, 1)):
                v = jnp.where((me & bit) != 0, jnp.flip(v, axis), v)
            return v.reshape(t // 128, 128)

        m_loc, s_loc_sum = by_device(m_slot), by_device(s_slot)

        lab_own = jnp.where(loss_mask > 0.0, labels, -1).astype(F32).reshape(nc, 128)
        stat_rows = t // 128
        packed = jnp.concatenate([m_loc, s_loc_sum, lab_own, jnp.zeros((8 - nc % 8, 128), F32)], axis=0)
        compact = jax.ShapeDtypeStruct((stat_rows, 128), F32)
        m, a, lab, misc = exchange(
            packed,
            n,
            functools.partial(stats_post, stat_rows, nc),
            [compact, compact, compact, jax.ShapeDtypeStruct((16, 128), F32)],
            0,
            "stats_exchange",
        )
        col_start = (me * vl).astype(F32)

        def wide(v):
            return jnp.broadcast_to(v[:, :, None], (stat_rows, 128, 128)).reshape(n, nc, 128, 128)

        m4, a4, lab4 = wide(m), wide(a), wide(lab - col_start)
        z4 = z.reshape(n, nc, 128, vl)
        inv = misc[:8]
        dz4, dhs, hits = None, [], []
        for c in range(nc):
            dh_c, dz4, hit = grad_h_chunk(me_arr, z4, m4, a4, lab4, inv, w, dz4, c)
            hits.append(hit)
            dhs.append(lax.psum_scatter(dh_c, "vp", scatter_dimension=0, tiled=True))
        grad_w = grad_w_call(h, dz4.reshape(t, vl))
        grad_x, sums = norm_bwd(x, g, dhs)
        vecs = jnp.sum(sums.reshape(2, 8, d), axis=1).reshape(2 * d // 128, 128)
        packed2 = jnp.concatenate([vecs, sum(hits)], axis=0)
        vrows = 2 * d // 128
        out_vec, hit_tot = exchange(
            packed2,
            n,
            functools.partial(final_post, vrows),
            [jax.ShapeDtypeStruct((vrows, 128), F32), jax.ShapeDtypeStruct((8, 128), F32)],
            1,
            "final_exchange",
        )
        loss = (misc[8, 0] - hit_tot[0, 0]) * misc[0, 0]
        out_vec = out_vec.reshape(2, d)
        return loss.reshape(1), grad_x.reshape(hidden.shape), grad_w, out_vec[0], out_vec[1]

    tok_spec = P("vp", "dp")
    return jax.shard_map(
        per_device,
        mesh=mesh,
        in_specs=(P("vp", "dp", None), P(None), P(None), P(None, "vp"), tok_spec, tok_spec),
        out_specs=(P("dp"), P("vp", "dp", None), P("dp", "vp"), P("dp"), P("dp")),
        check_vma=False,
    )
```
